32 devices in a mesh: rows: 8 (over z, x), grp: 4 (over y, core).
Axes of the slice: x: 2, y: 2, z: 4, core: 2. Of those that a mesh axis runs over, the one named last changes fastest.
Arguments:
- visibilities: float32 [2, 131072], P(None, ('rows', 'grp')), may hold values from -6 to 6
- uv_tiles: int32 [2, 131072], P(None, ('rows', 'grp')), may hold values from 0 to 511, as said below
- kernel_offsets: int32 [2, 131072], P(None, ('rows', 'grp')), may hold values from 0 to 7
- kernel: float32 [8, 8], replicated, may hold values from 0.5 to 1.5
Outputs:
- dirty_image: float32 [2, 4096, 4096], P(None, ('rows', 'grp'))
The draws below stay inside these ranges and needn't reach their ends.
Inputs may be any that keep to these rules, and one draw needn't show every extreme that they name: `uv_tiles`: row 0 holds tile rows, row 1 tile columns. The visibilities of baseline block q (positions q * 4096 to (q + 1) * 4096 - 1), with s = q divided by the number of devices of grp, have tile rows from s * 64 to (s + 1) * 64 - 1.
All inputs are finite; a program needn't handle non-finite values.
Results may differ from the reference program's by a relative error of at most 0.0044.
Values sent between devices are 32-bit elements; how exact they have to be, the bound alone decides.
A program may use at most 128 MiB of HBM per device.

```python
import jax
import jax.numpy as jnp
from jax import lax

G = 4096
TAPS = 8
VIS_DEV = 4096
VIS = 131072
SLAB = 512
N_GRP = 4


def draw_uv_tiles(key, part):
    first_key, second_key = jax.random.split(jax.random.fold_in(key, 17))
    position = jnp.arange(VIS, dtype=jnp.int32)
    slab_index = position // (VIS_DEV * N_GRP)
    tiles_slab = SLAB // TAPS
    tile_rows = slab_index * tiles_slab + jax.random.randint(first_key, (VIS,), 0, tiles_slab, dtype=jnp.int32)
    tile_cols = jax.random.randint(second_key, (VIS,), 0, G // TAPS, dtype=jnp.int32)
    return jnp.stack([tile_rows, tile_cols]).astype(jnp.int32)


def plant(drawn, own_key, low, top_value):
    longest = drawn.shape.index(max(drawn.shape))
    spots = []
    for shift in (0, 1):
        where = [jax.random.randint(jax.random.fold_in(own_key, axis), (), 0, length) for axis, length in enumerate(drawn.shape)]
        where[longest] = (where[longest] + shift) % drawn.shape[longest]
        spots.append(tuple(where))
    return drawn.at[spots[0]].set(low).at[spots[1]].set(top_value)


def level_of(own_key, extent, cuts, low, top_value):
    gain, own = 1.0, jax.random.fold_in(own_key, 6)
    for axis_at, blocks in cuts:
        heights = jnp.exp(jax.random.uniform(jax.random.fold_in(own, axis_at), (blocks,), jnp.float32, low / len(cuts), top_value / len(cuts)))
        gain = gain * jnp.repeat(heights, extent[axis_at] // blocks).reshape([-1 if axis == axis_at else 1 for axis in range(len(extent))])
    return gain


def noise(stream_key, extent, scale, limit, cuts=(), kind=jnp.bfloat16):
    values = scale * jax.random.normal(stream_key, extent, jnp.float32)
    if cuts:
        values = values * level_of(stream_key, extent, cuts, -0.22, 0.18)
    return jnp.clip(values, -limit, limit).astype(kind)


def setup_inputs(seed: int = 0) -> dict:
    splits = jax.random.split(jax.random.key(seed), 5)
    visibilities = noise(splits[0], (2, VIS), 1.0, 6.0, ((1, 32),), jnp.float32)
    uv_tiles = draw_uv_tiles(jax.random.fold_in(splits[4], 71), 0)
    kernel_offsets = plant(jax.random.randint(splits[2], (2, VIS), 0, TAPS), jax.random.fold_in(splits[2], 1), 0, TAPS - 1).astype(jnp.int32)
    kernel = jnp.clip(jax.random.uniform(splits[3], (TAPS, TAPS), jnp.float32, 0.5, 1.5), 0.5, 1.5)
    return {"visibilities": visibilities, "uv_tiles": uv_tiles, "kernel_offsets": kernel_offsets, "kernel": kernel}


def reference(visibilities, uv_tiles, kernel_offsets, kernel):
    tap_count = kernel.shape[0]
    row_start = tap_count * uv_tiles[0] + kernel_offsets[0]
    col_start = tap_count * uv_tiles[1] + kernel_offsets[1]
    row_taps = lax.optimization_barrier(kernel[kernel_offsets[0]].astype(jnp.bfloat16)).astype(jnp.float32)
    col_taps = kernel[kernel_offsets[1]]
    col_real = lax.optimization_barrier((visibilities[0][:, None] * col_taps).astype(jnp.bfloat16)).astype(jnp.float32)
    col_imag = lax.optimization_barrier((visibilities[1][:, None] * col_taps).astype(jnp.bfloat16)).astype(jnp.float32)
    col_index = (col_start[:, None] + jnp.arange(tap_count, dtype=jnp.int32)[None, :]) % G
    grid_real = jnp.zeros((G, G), jnp.float32)
    grid_imag = jnp.zeros((G, G), jnp.float32)
    for tap_index in range(tap_count):
        row_index = ((row_start + tap_index) % G)[:, None]
        weight = row_taps[:, tap_index:tap_index + 1]
        grid_real = grid_real.at[row_index, col_index].add(weight * col_real)
        grid_imag = grid_imag.at[row_index, col_index].add(weight * col_imag)
    spectrum = jnp.fft.ifft2(grid_real + 1j * grid_imag) * G
    return jnp.stack([jnp.real(spectrum).T, jnp.imag(spectrum).T]).astype(jnp.float32)
```

```python
import functools
import math

import jax
import jax.numpy as jnp
from jax import lax
from jax.experimental import pallas as pl
from jax.experimental.pallas import tpu as pltpu
from jax.sharding import PartitionSpec as P

G = 4096
SEGMENT = 64
WINDOW = 16
vis_block = 1024


def phases(first, second, length):
    angles = (first * second % length).astype(jnp.float32) * (2.0 * math.pi / length)
    return jnp.cos(angles), jnp.sin(angles)


def periodic(window, tile):
    half = WINDOW // 2
    swapped = jnp.concatenate([window[half:], window[:half]], axis=0)
    pattern = jnp.where((tile & 1) == 1, swapped, window)
    upper = lax.broadcasted_iota(jnp.int32, window.shape, 0) // half
    block = (tile - upper + 1) >> 1
    return pattern.astype(jnp.bfloat16), block.astype(jnp.float32).astype(jnp.bfloat16)


def grid_kernel(group_count, steps_per_block, slab, lines, period, segments, data_ref, taps_ref, table_ref, out_ref, total):
    step = pl.program_id(0)
    side = total.shape[0] - WINDOW
    seg_blocks = SEGMENT // WINDOW + 1

    @pl.when(step == 0)
    def _():
        total[...] = jnp.zeros_like(total)

    slab_index = step // (steps_per_block * group_count)
    base = slab_index * slab
    vis_re = data_ref[0, 0:1, :]
    vis_im = data_ref[0, 1:2, :]
    row_start = data_ref[0, 2:3, :].astype(jnp.int32) - base
    col_start = data_ref[0, 3:4, :].astype(jnp.int32)
    count = vis_re.shape[1]
    shape = (WINDOW, count)
    row_offset, row_tile = row_start & 7, row_start >> 3
    col_offset, col_tile = col_start & 7, col_start >> 3
    row_window = jnp.zeros(shape, jnp.float32)
    col_window = jnp.zeros(shape, jnp.float32)
    for offset in range(taps_ref.shape[0]):
        taps = jnp.broadcast_to(taps_ref[offset], shape)
        row_window = jnp.where(row_offset == offset, taps, row_window)
        col_window = jnp.where(col_offset == offset, taps, col_window)
    zero = jnp.zeros(shape, jnp.bfloat16)

    per_segment = SEGMENT // 8
    col_low, col_seg = col_tile & (per_segment - 1), col_tile // per_segment
    pattern_re, col_block = periodic(vis_re * col_window, col_low)
    pattern_im, _ = periodic(vis_im * col_window, col_low)
    seg_delta = jnp.broadcast_to(col_seg, shape) - lax.broadcasted_iota(jnp.int32, shape, 0)
    seg_delta = seg_delta.astype(jnp.float32).astype(jnp.bfloat16)
    one = jnp.ones(shape, jnp.bfloat16)
    weights_re = [jnp.where(col_block == i, pattern_re, zero) for i in range(seg_blocks)]
    weights_im = [jnp.where(col_block == i, pattern_im, zero) for i in range(seg_blocks)]
    hot = [jnp.where(seg_delta == i * WINDOW, one, zero) for i in range(segments // WINDOW)]
    weights = jnp.concatenate(weights_re + weights_im + hot, axis=0)
    parts = seg_blocks * WINDOW
    inner = jnp.dot(
        table_ref[: 2 * lines, : 2 * parts], weights[: 2 * parts], preferred_element_type=jnp.float32
    )
    outer = jnp.dot(
        table_ref[2 * lines :, 2 * parts :], weights[2 * parts :], preferred_element_type=jnp.float32
    )
    turn_re, turn_im = outer[:period], outer[period:]
    reals, imags = [], []
    for first in range(0, lines, period):
        in_re = inner[first : first + period]
        in_im = inner[lines + first : lines + first + period]
        reals.append((in_re * turn_re - in_im * turn_im).astype(jnp.bfloat16))
        imags.append((in_re * turn_im + in_im * turn_re).astype(jnp.bfloat16))
    spectra = jnp.concatenate(reals + imags, axis=0)

    row_pattern, row_block = periodic(row_window, row_tile)
    row_weights = jnp.concatenate(
        [jnp.where(row_block == i, row_pattern, zero) for i in range(slab // WINDOW + 1)], axis=0
    )
    rows = pl.ds(pl.multiple_of(base, WINDOW), slab + WINDOW)
    total[rows, :] += lax.dot_general(
        row_weights, spectra, (((1,), (1,)), ((), ())), preferred_element_type=jnp.float32
    )

    @pl.when(step == pl.num_programs(0) - 1)
    def _():
        total[:WINDOW, :] += total[side:, :]
        out_ref[0] = total[:side, :lines]
        out_ref[1] = total[:side, lines:]


def line_spectra(gathered, kernel, first_line, lines, group_count, slab, side):
    device_count, _, vis_count = gathered.shape
    block = min(vis_block, vis_count)
    steps = vis_count // block
    segments = side // SEGMENT
    period = min(segments, lines)
    tap_count = kernel.shape[0]
    offsets = jnp.arange(tap_count)[:, None]
    places = jnp.arange(WINDOW)[None, :] - offsets
    inside = (places >= 0) & (places < tap_count)
    taps = jnp.where(inside, kernel[offsets, jnp.clip(places, 0, tap_count - 1)], 0.0)[:, :, None]

    line_ids = first_line + jnp.arange(lines, dtype=jnp.int32)[:, None]
    in_cos, in_sin = phases(line_ids, jnp.arange(SEGMENT + WINDOW, dtype=jnp.int32)[None, :], side)
    out_cos, out_sin = phases(line_ids[:period], jnp.arange(segments, dtype=jnp.int32)[None, :], segments)
    inner = jnp.block([[in_cos, -in_sin], [in_sin, in_cos]])
    outer = jnp.concatenate([out_cos, out_sin], axis=0)
    table = jnp.concatenate(
        [
            jnp.pad(inner, ((0, 0), (0, segments))),
            jnp.pad(outer, ((0, 0), (inner.shape[1], 0))),
        ],
        axis=0,
    ).astype(jnp.bfloat16)
    body = functools.partial(grid_kernel, group_count, steps, slab, lines, period, segments)
    return pl.pallas_call(
        body,
        grid=(device_count * steps,),
        in_specs=[
            pl.BlockSpec((1, 4, block), lambda i: (i // steps, 0, i % steps)),
            pl.BlockSpec(taps.shape, lambda i: (0, 0, 0)),
            pl.BlockSpec(table.shape, lambda i: (0, 0)),
        ],
        out_specs=pl.BlockSpec((2, side, lines), lambda i: (0, 0, 0)),
        out_shape=jax.ShapeDtypeStruct((2, side, lines), jnp.float32),
        scratch_shapes=[pltpu.VMEM((side + WINDOW, 2 * lines), jnp.float32)],
        compiler_params=pltpu.CompilerParams(vmem_limit_bytes=60 * 2**20),
        name="line_spectra",
    )(gathered, taps, table)


def row_transform(spectra, lines, side):
    high = 128
    low = side // high
    grouped = spectra.reshape(2, high, low, lines)
    ids = jnp.arange(high, dtype=jnp.int32)
    cos, sin = phases(ids[:, None], ids[None, :], high)
    first = jnp.stack([jnp.stack([cos, sin]), jnp.stack([-sin, cos])])
    turned = jnp.einsum("cubl,ceuk->eblk", grouped, first, precision=lax.Precision.HIGH)
    low_ids = jnp.arange(low, dtype=jnp.int32)
    tw_cos, tw_sin = phases(low_ids[:, None], ids[None, :], side)
    tw_cos, tw_sin = tw_cos[:, None, :], tw_sin[:, None, :]
    turned = jnp.stack(
        [turned[0] * tw_cos - turned[1] * tw_sin, turned[0] * tw_sin + turned[1] * tw_cos]
    )
    cos, sin = phases(low_ids[:, None], low_ids[None, :], low)
    second = jnp.stack([jnp.stack([cos, sin]), jnp.stack([-sin, cos])]) * (1.0 / side)
    image = jnp.einsum(
        "eblk,ecbq->clqk", turned, second, precision=lax.Precision.HIGH
    )
    return image.reshape(2, lines, side)


def shards(visibilities, uv_tiles, kernel_offsets, kernel):
    rows_count = lax.axis_size("rows")
    group_count = lax.axis_size("grp")
    tap_count = kernel.shape[0]
    side = G
    slab = side // rows_count
    lines = slab // group_count
    starts = (tap_count * uv_tiles + kernel_offsets).astype(jnp.float32)
    packed = jnp.concatenate([visibilities, starts], axis=0)
    gathered = lax.all_gather(packed, ("rows", "grp"), axis=0, tiled=False)
    first_line = (lax.axis_index("rows") * group_count + lax.axis_index("grp")) * lines
    spectra = line_spectra(gathered, kernel, first_line, lines, group_count, slab, side)
    return row_transform(spectra, lines, side)


def solution(mesh):
    in_specs = (P(None, ("rows", "grp")), P(None, ("rows", "grp")), P(None, ("rows", "grp")), P())
    out_specs = P(None, ("rows", "grp"), None)
    return jax.shard_map(shards, mesh=mesh, in_specs=in_specs, out_specs=out_specs, check_vma=False)
```

```python
import functools
import math

import jax
import jax.numpy as jnp
from jax import lax
from jax.experimental import pallas as pl
from jax.experimental.pallas import tpu as pltpu
from jax.sharding import PartitionSpec as P

G = 4096
SEGMENT = 64
WINDOW = 16
vis_block = 2048


def phases(first, second, length):
    angles = (first * second % length).astype(jnp.float32) * (2.0 * math.pi / length)
    return jnp.cos(angles), jnp.sin(angles)


def periodic(window, tile):
    half = WINDOW // 2
    swapped = jnp.concatenate([window[half:], window[:half]], axis=0)
    pattern = jnp.where((tile & 1) == 1, swapped, window)
    upper = lax.broadcasted_iota(jnp.int32, window.shape, 0) // half
    block = (tile - upper + 1) >> 1
    return pattern.astype(jnp.bfloat16), block.astype(jnp.float32).astype(jnp.bfloat16)


def grid_kernel(group_count, steps_per_block, slab, lines, period, segments, data_ref, taps_ref, table_ref, out_ref, total):
    step = pl.program_id(0)
    side = total.shape[0] - WINDOW
    seg_blocks = SEGMENT // WINDOW + 1

    @pl.when(step == 0)
    def _():
        total[...] = jnp.zeros_like(total)

    slab_index = step // (steps_per_block * group_count)
    base = slab_index * slab
    vis_re = data_ref[0, 0:1, :]
    vis_im = data_ref[0, 1:2, :]
    row_start = data_ref[0, 2:3, :].astype(jnp.int32) - base
    col_start = data_ref[0, 3:4, :].astype(jnp.int32)
    count = vis_re.shape[1]
    shape = (WINDOW, count)
    row_offset, row_tile = row_start & 7, row_start >> 3
    col_offset, col_tile = col_start & 7, col_start >> 3
    row_window = jnp.zeros(shape, jnp.float32)
    col_window = jnp.zeros(shape, jnp.float32)
    for offset in range(taps_ref.shape[0]):
        taps = jnp.broadcast_to(taps_ref[offset], shape)
        row_window = jnp.where(row_offset == offset, taps, row_window)
        col_window = jnp.where(col_offset == offset, taps, col_window)
    zero = jnp.zeros(shape, jnp.bfloat16)

    per_segment = SEGMENT // 8
    col_low, col_seg = col_tile & (per_segment - 1), col_tile // per_segment
    pattern_re, col_block = periodic(vis_re * col_window, col_low)
    pattern_im, _ = periodic(vis_im * col_window, col_low)
    seg_delta = jnp.broadcast_to(col_seg, shape) - lax.broadcasted_iota(jnp.int32, shape, 0)
    seg_delta = seg_delta.astype(jnp.float32).astype(jnp.bfloat16)
    one = jnp.ones(shape, jnp.bfloat16)
    weights_re = [jnp.where(col_block == i, pattern_re, zero) for i in range(seg_blocks)]
    weights_im = [jnp.where(col_block == i, pattern_im, zero) for i in range(seg_blocks)]
    hot = [jnp.where(seg_delta == i * WINDOW, one, zero) for i in range(segments // WINDOW)]
    weights = jnp.concatenate(weights_re + weights_im + hot, axis=0)
    parts = seg_blocks * WINDOW
    inner = jnp.dot(
        table_ref[: 2 * lines, : 2 * parts], weights[: 2 * parts], preferred_element_type=jnp.float32
    )
    outer = jnp.dot(
        table_ref[2 * lines :, 2 * parts :], weights[2 * parts :], preferred_element_type=jnp.float32
    )
    turn_re, turn_im = outer[:period], outer[period:]
    reals, imags = [], []
    for first in range(0, lines, period):
        in_re = inner[first : first + period]
        in_im = inner[lines + first : lines + first + period]
        reals.append((in_re * turn_re - in_im * turn_im).astype(jnp.bfloat16))
        imags.append((in_re * turn_im + in_im * turn_re).astype(jnp.bfloat16))
    spectra = jnp.concatenate(reals + imags, axis=0)

    row_pattern, row_block = periodic(row_window, row_tile)
    row_weights = jnp.concatenate(
        [jnp.where(row_block == i, row_pattern, zero) for i in range(slab // WINDOW + 1)], axis=0
    )
    rows = pl.ds(pl.multiple_of(base, WINDOW), slab + WINDOW)
    total[rows, :] += lax.dot_general(
        row_weights, spectra, (((1,), (1,)), ((), ())), preferred_element_type=jnp.float32
    )

    @pl.when(step == pl.num_programs(0) - 1)
    def _():
        total[:WINDOW, :] += total[side:, :]
        out_ref[0] = total[:side, :lines]
        out_ref[1] = total[:side, lines:]


def line_spectra(gathered, kernel, first_line, lines, group_count, slab, side):
    device_count, _, vis_count = gathered.shape
    block = min(vis_block, vis_count)
    steps = vis_count // block
    segments = side // SEGMENT
    period = min(segments, lines)
    tap_count = kernel.shape[0]
    offsets = jnp.arange(tap_count)[:, None]
    places = jnp.arange(WINDOW)[None, :] - offsets
    inside = (places >= 0) & (places < tap_count)
    taps = jnp.where(inside, kernel[offsets, jnp.clip(places, 0, tap_count - 1)], 0.0)[:, :, None]

    line_ids = first_line + jnp.arange(lines, dtype=jnp.int32)[:, None]
    in_cos, in_sin = phases(line_ids, jnp.arange(SEGMENT + WINDOW, dtype=jnp.int32)[None, :], side)
    out_cos, out_sin = phases(line_ids[:period], jnp.arange(segments, dtype=jnp.int32)[None, :], segments)
    inner = jnp.block([[in_cos, -in_sin], [in_sin, in_cos]])
    outer = jnp.concatenate([out_cos, out_sin], axis=0)
    table = jnp.concatenate(
        [
            jnp.pad(inner, ((0, 0), (0, segments))),
            jnp.pad(outer, ((0, 0), (inner.shape[1], 0))),
        ],
        axis=0,
    ).astype(jnp.bfloat16)
    body = functools.partial(grid_kernel, group_count, steps, slab, lines, period, segments)
    return pl.pallas_call(
        body,
        grid=(device_count * steps,),
        in_specs=[
            pl.BlockSpec((1, 4, block), lambda i: (i // steps, 0, i % steps)),
            pl.BlockSpec(taps.shape, lambda i: (0, 0, 0)),
            pl.BlockSpec(table.shape, lambda i: (0, 0)),
        ],
        out_specs=pl.BlockSpec((2, side, lines), lambda i: (0, 0, 0)),
        out_shape=jax.ShapeDtypeStruct((2, side, lines), jnp.float32),
        scratch_shapes=[pltpu.VMEM((side + WINDOW, 2 * lines), jnp.float32)],
        compiler_params=pltpu.CompilerParams(vmem_limit_bytes=60 * 2**20),
        name="line_spectra",
    )(gathered, taps, table)


def row_transform(spectra, lines, side):
    high = 128
    low = side // high
    grouped = spectra.reshape(2, high, low, lines)
    ids = jnp.arange(high, dtype=jnp.int32)
    cos, sin = phases(ids[:, None], ids[None, :], high)
    first = jnp.stack([jnp.stack([cos, sin]), jnp.stack([-sin, cos])])
    turned = jnp.einsum("cubl,ceuk->eblk", grouped, first, precision=lax.Precision.HIGH)
    low_ids = jnp.arange(low, dtype=jnp.int32)
    tw_cos, tw_sin = phases(low_ids[:, None], ids[None, :], side)
    tw_cos, tw_sin = tw_cos[:, None, :], tw_sin[:, None, :]
    turned = jnp.stack(
        [turned[0] * tw_cos - turned[1] * tw_sin, turned[0] * tw_sin + turned[1] * tw_cos]
    )
    cos, sin = phases(low_ids[:, None], low_ids[None, :], low)
    second = jnp.stack([jnp.stack([cos, sin]), jnp.stack([-sin, cos])]) * (1.0 / side)
    image = jnp.einsum(
        "eblk,ecbq->clqk", turned, second, precision=lax.Precision.HIGH
    )
    return image.reshape(2, lines, side)


def shards(visibilities, uv_tiles, kernel_offsets, kernel):
    rows_count = lax.axis_size("rows")
    group_count = lax.axis_size("grp")
    tap_count = kernel.shape[0]
    side = G
    slab = side // rows_count
    lines = slab // group_count
    starts = (tap_count * uv_tiles + kernel_offsets).astype(jnp.float32)
    packed = jnp.concatenate([visibilities, starts], axis=0)
    gathered = lax.all_gather(packed, ("rows", "grp"), axis=0, tiled=False)
    first_line = (lax.axis_index("rows") * group_count + lax.axis_index("grp")) * lines
    spectra = line_spectra(gathered, kernel, first_line, lines, group_count, slab, side)
    return row_transform(spectra, lines, side)


def solution(mesh):
    in_specs = (P(None, ("rows", "grp")), P(None, ("rows", "grp")), P(None, ("rows", "grp")), P())
    out_specs = P(None, ("rows", "grp"), None)
    return jax.shard_map(shards, mesh=mesh, in_specs=in_specs, out_specs=out_specs, check_vma=False)
```
